32 devices in a mesh: sub: 32 (over z, y, x, core).
Axes of the slice: x: 2, y: 2, z: 4, core: 2. Of those that a mesh axis runs over, the one named last changes fastest.
Arguments:
- right_side: float32 [128, 128, 512], P('sub'), may hold values from -8 to 8
- sigma: float32 [128, 128, 512], P('sub'), may hold values from 0.25 to 2
- wind: float32 [128, 128, 512], P('sub'), may hold values from -0.8 to 0.8
- local_inverse: float32 [32, 512, 512], P('sub'), may hold values from -1 to 2, as said below
- basis_y: float32 [128, 32], replicated, may hold values from -0.5 to 0.5
- basis_z: float32 [512, 64], replicated, may hold values from -0.25 to 0.25
- gamma: float32 [5, 32, 64], replicated, may hold values from 0.3 to 3
Outputs:
- solution_field: float32 [128, 128, 512], P('sub')
- residual: float32 [128, 128, 512], P('sub')
The draws below stay inside these ranges and needn't reach their ends.
Inputs may be any that keep to these rules, and one draw needn't show every extreme that they name: `local_inverse`: each block is the identity plus a perturbation whose entries lie within 2/sqrt(512) of zero; each row of the perturbation has norm about one half.
All inputs are finite; a program needn't handle non-finite values.
Results may differ from the reference program's by a relative error of at most 0.00022.
Values sent between devices are 32-bit elements; how exact they have to be, the bound alone decides.
A program may use at most 64 MiB of HBM per device.

```python
import math
import jax
import jax.numpy as jnp
from jax import lax

CX = 4
NY = 128
NZ = 512
KY = 32
KZ = 64
BLOCKS = 32
NX = 128
LEVELS = 5
N_SUB = 32


def draw_local_inverse(key, part):
    noise = jnp.clip(jax.random.normal(key, (BLOCKS, NZ, NZ), jnp.float32), -4.0, 4.0)
    scaled = noise * (0.5 / jnp.sqrt(jnp.float32(NZ)))
    return scaled + jnp.eye(NZ, dtype=jnp.float32)[None]


def block_scale(own_key, shape, split, low, top_value):
    def one(axis_at, shards_of):
        steps = jax.random.uniform(jax.random.fold_in(jax.random.fold_in(own_key, 6), axis_at), (shards_of,), jnp.float32, low / len(split), top_value / len(split))
        return jnp.repeat(jnp.exp(steps), shape[axis_at] // shards_of).reshape((-1,) + (1,) * (len(shape) - axis_at - 1))

    gain = one(*split[0])
    for cut in split[1:]:
        gain = gain * one(*cut)
    return gain


def bell_draw(key, extent, deviation, reach, pieces=(), held_as=jnp.bfloat16):
    loudness = block_scale(key, extent, pieces, -0.22, 0.18) if pieces else 1.0
    result = jax.random.normal(key, extent, jnp.float32) * deviation * loudness
    return jnp.minimum(jnp.maximum(result, -reach), reach).astype(held_as)


def setup_inputs(seed: int = 0) -> dict:
    key_list = jax.random.split(jax.random.key(seed), 8)
    return {
        "right_side": bell_draw(key_list[0], (NX, NY, NZ), 1.0, 8.0, ((0, 32),), jnp.float32),
        "sigma": jnp.clip(0.25 + 1.75 * jax.random.uniform(key_list[1], (NX, NY, NZ), jnp.float32) ** block_scale(key_list[1], (NX, NY, NZ), ((0, 32),), -0.2, 0.2), 0.25, 2.0),
        "wind": jnp.clip(jax.random.uniform(key_list[2], (NX, NY, NZ), jnp.float32, -0.8, 0.8) * block_scale(key_list[2], (NX, NY, NZ), ((0, 32),), -0.4, 0.0), -0.8, 0.8),
        "local_inverse": draw_local_inverse(jax.random.fold_in(key_list[7], 71), 0),
        "basis_y": bell_draw(key_list[4], (NY, KY), NY ** -0.5, 0.5, (), jnp.float32),
        "basis_z": bell_draw(key_list[5], (NZ, KZ), NZ ** -0.5, 0.25, (), jnp.float32),
        "gamma": jnp.clip(jnp.exp(jax.random.uniform(key_list[6], (LEVELS, KY, KZ), jnp.float32, math.log(0.3), math.log(3.0))), 0.3, 3.0),
    }


HIGH = lax.Precision.HIGHEST

def apply_operator(field, sigma, wind):
    padded_x = jnp.pad(field, ((1, 1), (0, 0), (0, 0)))
    upper = padded_x[2:]
    lower = padded_x[:-2]
    padded_y = jnp.pad(field, ((0, 0), (1, 1), (0, 0)))
    padded_z = jnp.pad(field, ((0, 0), (0, 0), (1, 1)))
    beside = upper + lower + padded_y[:, 2:] + padded_y[:, :-2] + padded_z[:, :, 2:] + padded_z[:, :, :-2]
    return (6.0 + sigma) * field - beside + wind * (upper - lower)

def precondition(field, local_inverse, basis_y, basis_z, gamma):
    blocks = field.reshape(N_SUB, CX, NY, NZ)
    local = jnp.einsum('bxyz,bzw->bxyw', blocks, local_inverse, precision=HIGH)
    summed = lax.optimization_barrier(jnp.sum(blocks, axis=1))
    half = jnp.einsum('byz,zm->bym', summed, basis_z, precision=HIGH)
    proj = jnp.einsum('yk,bym->bkm', basis_y, half, precision=HIGH)
    coarse = jnp.zeros((N_SUB, KY, KZ), jnp.float32)
    for level in range(LEVELS):
        width = 2 ** (level + 1)
        grouped = lax.optimization_barrier(jnp.sum(proj.reshape(N_SUB // width, width, KY, KZ), axis=1, keepdims=True))
        grouped = jnp.broadcast_to(grouped, (N_SUB // width, width, KY, KZ)).reshape(N_SUB, KY, KZ)
        coarse = coarse + gamma[level] * grouped / jnp.sqrt(jnp.float32(CX * width))
    back = jnp.einsum('bkm,zm->bkz', coarse, basis_z, precision=HIGH)
    spread = jnp.einsum('yk,bkz->byz', basis_y, back, precision=HIGH)
    return (local + spread[:, None]).reshape(NX, NY, NZ)

def reference(right_side, sigma, wind, local_inverse, basis_y, basis_z, gamma):

    def inner(left, right):
        return jnp.sum(left * right)
    beta = jnp.sqrt(inner(right_side, right_side))
    first = right_side / beta
    z_one = precondition(first, local_inverse, basis_y, basis_z, gamma)
    image = apply_operator(z_one, sigma, wind)
    h11 = inner(first, image)
    image = image - h11 * first
    h21 = jnp.sqrt(inner(image, image))
    second = image / h21
    z_two = precondition(second, local_inverse, basis_y, basis_z, gamma)
    image = apply_operator(z_two, sigma, wind)
    h12 = inner(first, image)
    h22 = inner(second, image)
    image = image - h12 * first - h22 * second
    h32 = jnp.sqrt(inner(image, image))
    m11 = h11 * h11 + h21 * h21
    m12 = h11 * h12 + h21 * h22
    m22 = h12 * h12 + h22 * h22 + h32 * h32
    q_one = h11 * beta
    q_two = h12 * beta
    determ = m11 * m22 - m12 * m12
    y_one = (m22 * q_one - m12 * q_two) / determ
    y_two = (m11 * q_two - m12 * q_one) / determ
    solution_field = y_one * z_one + y_two * z_two
    residual = right_side - apply_operator(solution_field, sigma, wind)
    return (solution_field, residual)
```

```python
import functools

import jax
import jax.numpy as jnp
from jax import lax
from jax.experimental import pallas as pl
from jax.experimental.pallas import tpu as pltpu
from jax.sharding import PartitionSpec as P

HIGH = lax.Precision.HIGHEST
MESH = pl.DeviceIdType.MESH
PAD = 8


def split(x):
    hi = x.astype(jnp.bfloat16)
    lo = (x - hi.astype(jnp.float32)).astype(jnp.bfloat16)
    return hi, lo


def mm(a, b):
    return jnp.dot(a, b, preferred_element_type=jnp.float32)


def mt(a, b):
    return lax.dot_general(
        a, b, (((1,), (1,)), ((), ())), preferred_element_type=jnp.float32
    )


def tm(a, b):
    return lax.dot_general(
        a, b, (((0,), (0,)), ((), ())), preferred_element_type=jnp.float32
    )


def fold(x):
    part = jnp.sum(x, axis=0, keepdims=True)
    out = part[:, 0:128]
    for at in range(128, part.shape[1], 128):
        out = out + part[:, at : at + 128]
    return out


def kernel(
    n, block,
    r_hbm, sg_hbm, wd_hbm, li_hbm, by_hbm, bz_hbm, gm_hbm,
    x_hbm, res_hbm,
    r, sg, wd, lf, by, bz, gm, lh, ll, u1, u2, w1, w2, hs, hr, xo, ro,
    own, gat, tot, allb, low_s, low_r, nbr, gs, ggat, gtot, gall,
    in_sem, out_sem, sa, ra, sb, rb, se, re, sh, rh, sga, rga, sgb, rgb,
):
    layers, rows, depth = r.shape
    ky = by.shape[0]
    half = ky // 2
    kz = bz.shape[0]
    levels = gm.shape[0]
    blocks = n // block
    low_levels = block.bit_length() - 1
    me = lax.axis_index("sub")
    p = lax.rem(me, block)
    z = lax.div(me, block)
    us = (u1, u2)
    ws = (w1, w2)

    def load(i, src, dst):
        c = pltpu.make_async_copy(src, dst, in_sem.at[i])
        c.start()
        return c

    c_r = load(0, r_hbm, r)
    c_bz = load(1, bz_hbm, bz)
    c_by = load(2, by_hbm, by)
    c_l = load(3, li_hbm, lf)
    c_gm = load(4, gm_hbm, gm)
    c_sg = load(5, sg_hbm, sg)
    c_wd = load(6, wd_hbm, wd)

    barrier = pltpu.get_barrier_semaphore()
    in_block = [z * block + lax.rem(p + d, block) for d in range(1, block)]
    across = [lax.rem(z + d, blocks) * block + p for d in range(1, blocks)]
    first_cross = jnp.logical_and(p == 0, z > 0)
    last_cross = jnp.logical_and(p == block - 1, z < blocks - 1)

    def signal(target):
        pl.semaphore_signal(barrier, inc=1, device_id=(target,), device_id_type=MESH)

    for target in in_block + across:
        signal(target)

    @pl.when(first_cross)
    def _():
        signal(me - 1)

    @pl.when(last_cross)
    def _():
        signal(me + 1)

    zero_rows = jnp.zeros((PAD, depth), jnp.float32)
    for u in us:
        for l in range(1, layers + 1):
            u[l, 0:PAD, :] = zero_rows
            u[l, PAD + rows : PAD + rows + PAD, :] = zero_rows

    @pl.when(me == 0)
    def _():
        for k in range(2):
            us[k][0, PAD : PAD + rows, :] = jnp.zeros((rows, depth), jnp.float32)

    @pl.when(me == n - 1)
    def _():
        for k in range(2):
            us[k][layers + 1, PAD : PAD + rows, :] = jnp.zeros((rows, depth), jnp.float32)

    def send(src, dst, s, q, target):
        return pltpu.make_async_remote_copy(
            src_ref=src, dst_ref=dst, send_sem=s, recv_sem=q,
            device_id=(target,), device_id_type=MESH,
        )

    def project(k, field):
        summed = field[0]
        for l in range(1, layers):
            summed = summed + field[l]
        sh_, sl_ = split(summed)
        bh, bl = split(bz[...])
        part = mt(sh_, bh) + mt(sl_, bh) + mt(sh_, bl)
        full = jnp.dot(
            by[...], part, precision=HIGH, preferred_element_type=jnp.float32
        )
        packed = jnp.concatenate([full[0:half], full[half:ky]], axis=1)
        own[k] = packed
        gat[k, p] = packed

    def a_copy(k, d):
        return send(own.at[k], gat.at[k, p], sa.at[k, d], ra.at[k, p], in_block[d - 1])

    def a_arrived(k, d):
        q = lax.rem(p + d, block)
        return send(own.at[k], gat.at[k, q], sa.at[k, d], ra.at[k, q], in_block[d - 1])

    def b_copy(k, d):
        return send(tot.at[k], allb.at[k, z], sb.at[k, d], rb.at[k, z], across[d - 1])

    def b_arrived(k, d):
        q = lax.rem(z + d, blocks)
        return send(tot.at[k], allb.at[k, q], sb.at[k, d], rb.at[k, q], across[d - 1])

    def down(k):
        return send(hs.at[k, 0], hr.at[k, 1], sh.at[k, 0], rh.at[k, 1], me - 1)

    def up(k):
        return send(hs.at[k, 1], hr.at[k, 0], sh.at[k, 1], rh.at[k, 0], me + 1)

    def low_down(k):
        return send(low_s.at[k, 0], low_r.at[k, 1], se.at[k, 0], re.at[k, 1], me - block)

    def low_up(k):
        return send(low_s.at[k, 1], low_r.at[k, 0], se.at[k, 1], re.at[k, 0], me + block)

    def local(x):
        xh, xl = split(x)
        return mm(xh, lh[...]) + mm(xl, lh[...]) + mm(xh, ll[...])

    def factor(level):
        g = gm[level]
        return jnp.concatenate([g[0:half], g[half:ky]], axis=1) * (
            (layers * 2 ** (level + 1)) ** -0.5
        )

    def low_part(k, q, upper):
        out = None
        for level in range(low_levels):
            width = 2 ** (level + 1)
            start = lax.div(q, width) * width
            if width == block:
                acc = tot[k]
            else:
                acc = gat[k, start]
                for j in range(1, width):
                    acc = acc + gat[k, start + j]
            term = upper[level] * acc
            out = term if out is None else out + term
        return out

    def high_part(k, zz, upper):
        out = jnp.zeros(tot.shape[1:], jnp.float32)
        for level in range(low_levels, levels):
            width = 2 ** (level + 1) // block
            start = lax.div(zz, width) * width
            acc = allb[k, start]
            for j in range(1, width):
                acc = acc + allb[k, start + j]
            out = out + upper[level] * acc
        return out

    def boundary(k, field):
        first = local(field[0])
        hs[k, 0] = first

        @pl.when(me > 0)
        def _():
            down(k).start()

        us[k][1, PAD : PAD + rows, :] = first
        last = local(field[layers - 1])
        hs[k, 1] = last

        @pl.when(me < n - 1)
        def _():
            up(k).start()

        us[k][layers, PAD : PAD + rows, :] = last

    def middle(k, field):
        for l in range(1, layers - 1):
            us[k][l + 1, PAD : PAD + rows, :] = local(field[l])

    def exchange(k):
        fac = [factor(level) for level in range(levels)]
        for d in range(1, block):
            a_arrived(k, d).wait_recv()
        acc = gat[k, 0]
        for j in range(1, block):
            acc = acc + gat[k, j]
        tot[k] = acc
        allb[k, z] = acc
        for d in range(1, blocks):
            b_copy(k, d).start()

        @pl.when(jnp.logical_and(p == block - 1, z > 0))
        def _():
            low_s[k, 0] = low_part(k, 0, fac)
            low_down(k).start()

        @pl.when(jnp.logical_and(p == 0, z < blocks - 1))
        def _():
            low_s[k, 1] = low_part(k, block - 1, fac)
            low_up(k).start()

        nbr[1] = low_part(k, p, fac)

        @pl.when(p > 0)
        def _():
            nbr[0] = low_part(k, p - 1, fac)

        @pl.when(p < block - 1)
        def _():
            nbr[2] = low_part(k, p + 1, fac)

        @pl.when(jnp.logical_and(p == 0, z == 0))
        def _():
            nbr[0] = jnp.zeros(nbr.shape[1:], jnp.float32)

        @pl.when(jnp.logical_and(p == block - 1, z == blocks - 1))
        def _():
            nbr[2] = jnp.zeros(nbr.shape[1:], jnp.float32)

        for d in range(1, blocks):
            b_arrived(k, d).wait_recv()

        @pl.when(first_cross)
        def _():
            low_up(k).wait_recv()
            nbr[0] = low_r[k, 0]

        @pl.when(last_cross)
        def _():
            low_down(k).wait_recv()
            nbr[2] = low_r[k, 1]

        here = high_part(k, z, fac)
        before = high_part(k, lax.div(lax.rem(me + n - 1, n), block), fac)
        after = high_part(k, lax.div(lax.rem(me + 1, n), block), fac)
        three = []
        for c in (nbr[0] + before, nbr[1] + here, nbr[2] + after):
            three += [c[:, 0:kz], c[:, kz : 2 * kz]]
        stack = jnp.concatenate(three, axis=0)
        back = jnp.dot(
            stack, bz[...], precision=HIGH, preferred_element_type=jnp.float32
        )
        bh, bl = split(by[...])
        spreads = []
        for j in range(3):
            th, tl = split(back[j * ky : (j + 1) * ky])
            spreads.append(tm(bh, th) + tm(bl, th) + tm(bh, tl))
        u = us[k]
        mine = spreads[1]
        for l in range(1, layers + 1):
            u[l, PAD : PAD + rows, :] = u[l, PAD : PAD + rows, :] + mine
        u[0, PAD : PAD + rows, :] = jnp.where(me > 0, spreads[0], 0.0)
        u[layers + 1, PAD : PAD + rows, :] = jnp.where(me < n - 1, spreads[2], 0.0)

    step = 32

    def operator(k, l):
        u = us[k]
        col = lax.broadcasted_iota(jnp.int32, (step, depth), 1)
        for y in range(0, rows, step):
            a = PAD + y
            c = u[l + 1, a : a + step, :]
            hi = u[l + 2, a : a + step, :]
            lo = u[l, a : a + step, :]
            fwd = jnp.where(col == depth - 1, 0.0, pltpu.roll(c, depth - 1, 1))
            bwd = jnp.where(col == 0, 0.0, pltpu.roll(c, 1, 1))
            beside = (
                hi + lo + u[l + 1, a + 1 : a + step + 1, :]
                + u[l + 1, a - 1 : a + step - 1, :] + fwd + bwd
            )
            ws[k][l, y : y + step, :] = (
                (6.0 + sg[l, y : y + step, :]) * c - beside
                + wd[l, y : y + step, :] * (hi - lo)
            )

    def stencil(k):
        for l in range(1, layers - 1):
            operator(k, l)
        u = us[k]

        @pl.when(me > 0)
        def _():
            up(k).wait_recv()
            u[0, PAD : PAD + rows, :] = u[0, PAD : PAD + rows, :] + hr[k, 0]

        operator(k, 0)

        @pl.when(me < n - 1)
        def _():
            down(k).wait_recv()
            u[layers + 1, PAD : PAD + rows, :] = u[layers + 1, PAD : PAD + rows, :] + hr[k, 1]

        operator(k, layers - 1)

    def dots(pairs):
        out = []
        for a, b in pairs:
            acc = a[0] * b[0]
            for l in range(1, layers):
                acc = acc + a[l] * b[l]
            out.append(fold(acc))
        return out

    c_bz.wait()
    c_by.wait()
    c_r.wait()
    project(0, r)
    extra = jnp.where(first_cross, 1, 0) + jnp.where(last_cross, 1, 0)
    pl.semaphore_wait(barrier, block - 1 + blocks - 1 + extra)

    for d in range(1, block):
        a_copy(0, d).start()
    c_l.wait()
    big, small = split(lf[0])
    lh[...] = big
    ll[...] = small
    boundary(0, r)
    middle(0, r)
    c_gm.wait()
    exchange(0)
    c_sg.wait()
    c_wd.wait()
    stencil(0)

    project(1, w1)
    for d in range(1, block):
        a_copy(1, d).start()
    boundary(1, w1)
    middle(1, w1)
    early = dots([(r, r), (r, w1), (w1, w1)])
    exchange(1)
    stencil(1)

    late = dots([(r, w2), (w1, w2), (w2, w2)])
    blank = jnp.zeros((2, 128), jnp.float32)
    sums = jnp.concatenate(early + late + [blank], axis=0)
    gs[...] = sums
    ggat[p] = sums

    def ga_copy(d):
        return send(gs, ggat.at[p], sga.at[d], rga.at[p], in_block[d - 1])

    def ga_arrived(d):
        q = lax.rem(p + d, block)
        return send(gs, ggat.at[q], sga.at[d], rga.at[q], in_block[d - 1])

    def gb_copy(d):
        return send(gtot, gall.at[z], sgb.at[d], rgb.at[z], across[d - 1])

    def gb_arrived(d):
        q = lax.rem(z + d, blocks)
        return send(gtot, gall.at[q], sgb.at[d], rgb.at[q], across[d - 1])

    for d in range(1, block):
        ga_copy(d).start()
    for d in range(1, block):
        ga_arrived(d).wait_recv()
    acc = ggat[0]
    for j in range(1, block):
        acc = acc + ggat[j]
    gtot[...] = acc
    gall[z] = acc
    for d in range(1, blocks):
        gb_copy(d).start()
    for d in range(1, blocks):
        gb_arrived(d).wait_recv()
    acc = gall[0]
    for j in range(1, blocks):
        acc = acc + gall[j]
    full = jnp.sum(acc, axis=1, keepdims=True)
    g01, g11 = full[1:2], full[2:3]
    g02, g12, g22 = full[3:4], full[4:5], full[5:6]
    ratio = g12 / g11
    c2 = (g02 - ratio * g01) / (g22 - ratio * g12)
    c1 = g01 / g11 - ratio * c2
    outs = []
    for l in range(layers):
        for y in range(0, rows, step):
            a = PAD + y
            xo[l, y : y + step, :] = (
                c1 * u1[l + 1, a : a + step, :] + c2 * u2[l + 1, a : a + step, :]
            )
            ro[l, y : y + step, :] = (
                r[l, y : y + step, :]
                - c1 * w1[l, y : y + step, :] - c2 * w2[l, y : y + step, :]
            )
        cx = pltpu.make_async_copy(xo.at[l], x_hbm.at[l], out_sem.at[0, l])
        cr = pltpu.make_async_copy(ro.at[l], res_hbm.at[l], out_sem.at[1, l])
        cx.start()
        cr.start()
        outs += [cx, cr]

    for k in range(2):
        for d in range(1, block):
            a_copy(k, d).wait_send()
        for d in range(1, blocks):
            b_copy(k, d).wait_send()

        @pl.when(jnp.logical_and(p == block - 1, z > 0))
        def _():
            low_down(k).wait_send()

        @pl.when(jnp.logical_and(p == 0, z < blocks - 1))
        def _():
            low_up(k).wait_send()

        @pl.when(me > 0)
        def _():
            down(k).wait_send()

        @pl.when(me < n - 1)
        def _():
            up(k).wait_send()

    for d in range(1, block):
        ga_copy(d).wait_send()
    for d in range(1, blocks):
        gb_copy(d).wait_send()
    for c in outs:
        c.wait()


def on_device(right_side, sigma, wind, local_inverse, basis_y, basis_z, gamma):
    n = lax.axis_size("sub")
    block = min(8, n)
    blocks = n // block
    layers, rows, depth = right_side.shape
    ky = basis_y.shape[1]
    kz = basis_z.shape[1]
    levels = gamma.shape[0]
    f32 = jnp.float32
    packed = (ky // 2, 2 * kz)
    cube = pltpu.VMEM((layers, rows, depth), f32)
    padded = pltpu.VMEM((layers + 2, rows + 2 * PAD, depth), f32)
    dma = pltpu.SemaphoreType.DMA
    scratch = [
        cube, cube, cube,
        pltpu.VMEM((1, depth, depth), f32),
        pltpu.VMEM((ky, rows), f32),
        pltpu.VMEM((kz, depth), f32),
        pltpu.VMEM(gamma.shape, f32),
        pltpu.VMEM((depth, depth), jnp.bfloat16),
        pltpu.VMEM((depth, depth), jnp.bfloat16),
        padded, padded, cube, cube,
        pltpu.VMEM((2, 2, rows, depth), f32),
        pltpu.VMEM((2, 2, rows, depth), f32),
        cube, cube,
        pltpu.VMEM((2,) + packed, f32),
        pltpu.VMEM((2, block) + packed, f32),
        pltpu.VMEM((2,) + packed, f32),
        pltpu.VMEM((2, blocks) + packed, f32),
        pltpu.VMEM((2, 2) + packed, f32),
        pltpu.VMEM((2, 2) + packed, f32),
        pltpu.VMEM((3,) + packed, f32),
        pltpu.VMEM((8, 128), f32),
        pltpu.VMEM((block, 8, 128), f32),
        pltpu.VMEM((8, 128), f32),
        pltpu.VMEM((blocks, 8, 128), f32),
        dma((7,)), dma((2, layers)),
        dma((2, block)), dma((2, block)),
        dma((2, blocks)), dma((2, blocks)),
        dma((2, 2)), dma((2, 2)),
        dma((2, 2)), dma((2, 2)),
        dma((block,)), dma((block,)),
        dma((blocks,)), dma((blocks,)),
    ]
    anywhere = pl.BlockSpec(memory_space=pl.ANY)
    out = jax.ShapeDtypeStruct(right_side.shape, f32)
    return pl.pallas_call(
        functools.partial(kernel, n, block),
        out_shape=(out, out),
        in_specs=[anywhere] * 7,
        out_specs=(anywhere, anywhere),
        scratch_shapes=scratch,
        compiler_params=pltpu.CompilerParams(
            collective_id=0, has_side_effects=True, vmem_limit_bytes=56 * 2**20,
        ),
        name="gmres",
    )(right_side, sigma, wind, local_inverse, basis_y.T, basis_z.T, gamma)


def solution(mesh):
    placed = (
        P("sub", None, None),
        P("sub", None, None),
        P("sub", None, None),
        P("sub", None, None),
        P(),
        P(),
        P(),
    )
    return jax.shard_map(
        on_device,
        mesh=mesh,
        in_specs=placed,
        out_specs=(P("sub", None, None), P("sub", None, None)),
        check_vma=False,
    )
```

```python
import functools

import jax
import jax.numpy as jnp
from jax import lax
from jax.experimental import pallas as pl
from jax.experimental.pallas import tpu as pltpu
from jax.sharding import PartitionSpec as P

HIGH = lax.Precision.HIGHEST
MESH = pl.DeviceIdType.MESH
PAD = 8


def split(x):
    hi = x.astype(jnp.bfloat16)
    lo = (x - hi.astype(jnp.float32)).astype(jnp.bfloat16)
    return hi, lo


def mm(a, b):
    return jnp.dot(a, b, preferred_element_type=jnp.float32)


def mt(a, b):
    return lax.dot_general(
        a, b, (((1,), (1,)), ((), ())), preferred_element_type=jnp.float32
    )


def tm(a, b):
    return lax.dot_general(
        a, b, (((0,), (0,)), ((), ())), preferred_element_type=jnp.float32
    )


def fold(x):
    part = jnp.sum(x, axis=0, keepdims=True)
    out = part[:, 0:128]
    for at in range(128, part.shape[1], 128):
        out = out + part[:, at : at + 128]
    return out


def kernel(
    n, block,
    r_hbm, sg_hbm, wd_hbm, li_hbm, by_hbm, bz_hbm, gm_hbm,
    r, u1, u2, w1, w2, coef,
    sg, wd, lf, by, bz, gm, lh, ll, hs, hr,
    own, gat, tot, allb, low_s, low_r, nbr, gs, ggat,
    in_sem, sa, ra, sb, rb, se, re, sh, rh, sga, rga,
):
    layers, rows, depth = r.shape
    ky = by.shape[0]
    half = ky // 2
    kz = bz.shape[0]
    levels = gm.shape[0]
    blocks = n // block
    low_levels = block.bit_length() - 1
    me = lax.axis_index("sub")
    p = lax.rem(me, block)
    z = lax.div(me, block)
    us = (u1, u2)
    ws = (w1, w2)

    def load(i, src, dst):
        c = pltpu.make_async_copy(src, dst, in_sem.at[i])
        c.start()
        return c

    c_r = load(0, r_hbm, r)
    c_bz = load(1, bz_hbm, bz)
    c_by = load(2, by_hbm, by)
    c_l = load(3, li_hbm, lf)
    c_gm = load(4, gm_hbm, gm)
    c_sg = load(5, sg_hbm, sg)
    c_wd = load(6, wd_hbm, wd)

    barrier = pltpu.get_barrier_semaphore()
    in_block = [z * block + lax.rem(p + d, block) for d in range(1, block)]
    across = [lax.rem(z + d, blocks) * block + p for d in range(1, blocks)]
    first_cross = jnp.logical_and(p == 0, z > 0)
    last_cross = jnp.logical_and(p == block - 1, z < blocks - 1)

    def signal(target):
        pl.semaphore_signal(barrier, inc=1, device_id=(target,), device_id_type=MESH)

    for target in in_block + across:
        signal(target)

    @pl.when(first_cross)
    def _():
        signal(me - 1)

    @pl.when(last_cross)
    def _():
        signal(me + 1)

    zero_rows = jnp.zeros((PAD, depth), jnp.float32)
    for u in us:
        for l in range(1, layers + 1):
            u[l, 0:PAD, :] = zero_rows
            u[l, PAD + rows : PAD + rows + PAD, :] = zero_rows

    @pl.when(me == 0)
    def _():
        for k in range(2):
            us[k][0, PAD : PAD + rows, :] = jnp.zeros((rows, depth), jnp.float32)

    @pl.when(me == n - 1)
    def _():
        for k in range(2):
            us[k][layers + 1, PAD : PAD + rows, :] = jnp.zeros((rows, depth), jnp.float32)

    def send(src, dst, s, q, target):
        return pltpu.make_async_remote_copy(
            src_ref=src, dst_ref=dst, send_sem=s, recv_sem=q,
            device_id=(target,), device_id_type=MESH,
        )

    def project(k, field):
        summed = field[0]
        for l in range(1, layers):
            summed = summed + field[l]
        sh_, sl_ = split(summed)
        bh, bl = split(bz[...])
        part = mt(sh_, bh) + mt(sl_, bh) + mt(sh_, bl)
        full = jnp.dot(
            by[...], part, precision=HIGH, preferred_element_type=jnp.float32
        )
        packed = jnp.concatenate([full[0:half], full[half:ky]], axis=1)
        own[k] = packed
        gat[k, p] = packed

    def a_copy(k, d):
        return send(own.at[k], gat.at[k, p], sa.at[k, d], ra.at[k, p], in_block[d - 1])

    def a_arrived(k, d):
        q = lax.rem(p + d, block)
        return send(own.at[k], gat.at[k, q], sa.at[k, d], ra.at[k, q], in_block[d - 1])

    def b_copy(k, d):
        return send(tot.at[k], allb.at[k, z], sb.at[k, d], rb.at[k, z], across[d - 1])

    def b_arrived(k, d):
        q = lax.rem(z + d, blocks)
        return send(tot.at[k], allb.at[k, q], sb.at[k, d], rb.at[k, q], across[d - 1])

    def down(k):
        return send(hs.at[k, 0], hr.at[k, 1], sh.at[k, 0], rh.at[k, 1], me - 1)

    def up(k):
        return send(hs.at[k, 1], hr.at[k, 0], sh.at[k, 1], rh.at[k, 0], me + 1)

    def low_down(k):
        return send(low_s.at[k, 0], low_r.at[k, 1], se.at[k, 0], re.at[k, 1], me - block)

    def low_up(k):
        return send(low_s.at[k, 1], low_r.at[k, 0], se.at[k, 1], re.at[k, 0], me + block)

    def local(x):
        xh, xl = split(x)
        return mm(xh, lh[...]) + mm(xl, lh[...]) + mm(xh, ll[...])

    def factor(level):
        g = gm[level]
        return jnp.concatenate([g[0:half], g[half:ky]], axis=1) * (
            (layers * 2 ** (level + 1)) ** -0.5
        )

    def low_part(k, q, upper):
        out = None
        for level in range(low_levels):
            width = 2 ** (level + 1)
            start = lax.div(q, width) * width
            if width == block:
                acc = tot[k]
            else:
                acc = gat[k, start]
                for j in range(1, width):
                    acc = acc + gat[k, start + j]
            term = upper[level] * acc
            out = term if out is None else out + term
        return out

    def high_part(k, zz, upper):
        out = jnp.zeros(tot.shape[1:], jnp.float32)
        for level in range(low_levels, levels):
            width = 2 ** (level + 1) // block
            start = lax.div(zz, width) * width
            acc = allb[k, start]
            for j in range(1, width):
                acc = acc + allb[k, start + j]
            out = out + upper[level] * acc
        return out

    def edges(k, field):
        first = local(field[0])
        hs[k, 0] = first
        us[k][1, PAD : PAD + rows, :] = first
        last = local(field[layers - 1])
        hs[k, 1] = last
        us[k][layers, PAD : PAD + rows, :] = last

    def send_edges(k):
        @pl.when(me > 0)
        def _():
            down(k).start()

        @pl.when(me < n - 1)
        def _():
            up(k).start()

    def middle(k, field):
        for l in range(1, layers - 1):
            us[k][l + 1, PAD : PAD + rows, :] = local(field[l])

    def exchange(k):
        fac = [factor(level) for level in range(levels)]
        for d in range(1, block):
            a_arrived(k, d).wait_recv()
        acc = gat[k, 0]
        for j in range(1, block):
            acc = acc + gat[k, j]
        tot[k] = acc
        allb[k, z] = acc
        for d in range(1, blocks):
            b_copy(k, d).start()

        @pl.when(jnp.logical_and(p == block - 1, z > 0))
        def _():
            low_s[k, 0] = low_part(k, 0, fac)
            low_down(k).start()

        @pl.when(jnp.logical_and(p == 0, z < blocks - 1))
        def _():
            low_s[k, 1] = low_part(k, block - 1, fac)
            low_up(k).start()

        nbr[1] = low_part(k, p, fac)

        @pl.when(p > 0)
        def _():
            nbr[0] = low_part(k, p - 1, fac)

        @pl.when(p < block - 1)
        def _():
            nbr[2] = low_part(k, p + 1, fac)

        @pl.when(jnp.logical_and(p == 0, z == 0))
        def _():
            nbr[0] = jnp.zeros(nbr.shape[1:], jnp.float32)

        @pl.when(jnp.logical_and(p == block - 1, z == blocks - 1))
        def _():
            nbr[2] = jnp.zeros(nbr.shape[1:], jnp.float32)

        for d in range(1, blocks):
            b_arrived(k, d).wait_recv()

        @pl.when(first_cross)
        def _():
            low_up(k).wait_recv()
            nbr[0] = low_r[k, 0]

        @pl.when(last_cross)
        def _():
            low_down(k).wait_recv()
            nbr[2] = low_r[k, 1]

        here = high_part(k, z, fac)
        before = high_part(k, lax.div(lax.rem(me + n - 1, n), block), fac)
        after = high_part(k, lax.div(lax.rem(me + 1, n), block), fac)
        three = []
        for c in (nbr[0] + before, nbr[1] + here, nbr[2] + after):
            three += [c[:, 0:kz], c[:, kz : 2 * kz]]
        stack = jnp.concatenate(three, axis=0)
        back = jnp.dot(
            stack, bz[...], precision=HIGH, preferred_element_type=jnp.float32
        )
        bh, bl = split(by[...])
        spreads = []
        for j in range(3):
            th, tl = split(back[j * ky : (j + 1) * ky])
            spreads.append(tm(bh, th) + tm(bl, th) + tm(bh, tl))
        u = us[k]
        mine = spreads[1]
        for l in range(1, layers + 1):
            u[l, PAD : PAD + rows, :] = u[l, PAD : PAD + rows, :] + mine
        u[0, PAD : PAD + rows, :] = jnp.where(me > 0, spreads[0], 0.0)
        u[layers + 1, PAD : PAD + rows, :] = jnp.where(me < n - 1, spreads[2], 0.0)

    step = 32

    def operator(k, l):
        u = us[k]
        col = lax.broadcasted_iota(jnp.int32, (step, depth), 1)
        for y in range(0, rows, step):
            a = PAD + y
            c = u[l + 1, a : a + step, :]
            hi = u[l + 2, a : a + step, :]
            lo = u[l, a : a + step, :]
            fwd = jnp.where(col == depth - 1, 0.0, pltpu.roll(c, depth - 1, 1))
            bwd = jnp.where(col == 0, 0.0, pltpu.roll(c, 1, 1))
            beside = (
                hi + lo + u[l + 1, a + 1 : a + step + 1, :]
                + u[l + 1, a - 1 : a + step - 1, :] + fwd + bwd
            )
            ws[k][l, y : y + step, :] = (
                (6.0 + sg[l, y : y + step, :]) * c - beside
                + wd[l, y : y + step, :] * (hi - lo)
            )

    def stencil(k):
        for l in range(1, layers - 1):
            operator(k, l)
        u = us[k]

        @pl.when(me > 0)
        def _():
            up(k).wait_recv()
            u[0, PAD : PAD + rows, :] = u[0, PAD : PAD + rows, :] + hr[k, 0]

        operator(k, 0)

        @pl.when(me < n - 1)
        def _():
            down(k).wait_recv()
            u[layers + 1, PAD : PAD + rows, :] = u[layers + 1, PAD : PAD + rows, :] + hr[k, 1]

        operator(k, layers - 1)

    def dots(pairs):
        out = []
        for a, b in pairs:
            acc = a[0] * b[0]
            for l in range(1, layers):
                acc = acc + a[l] * b[l]
            out.append(fold(acc))
        return out

    c_bz.wait()
    c_by.wait()
    c_r.wait()
    project(0, r)
    c_l.wait()
    big, small = split(lf[0])
    lh[...] = big
    ll[...] = small
    edges(0, r)
    extra = jnp.where(first_cross, 1, 0) + jnp.where(last_cross, 1, 0)
    pl.semaphore_wait(barrier, block - 1 + blocks - 1 + extra)
    for d in range(1, block):
        a_copy(0, d).start()
    send_edges(0)
    middle(0, r)
    c_gm.wait()
    exchange(0)
    c_sg.wait()
    c_wd.wait()
    stencil(0)

    project(1, w1)
    for d in range(1, block):
        a_copy(1, d).start()
    edges(1, w1)
    send_edges(1)
    middle(1, w1)
    early = dots([(r, r), (r, w1), (w1, w1)])
    exchange(1)
    stencil(1)

    late = dots([(r, w2), (w1, w2), (w2, w2)])
    blank = jnp.zeros((2, 128), jnp.float32)
    sums = jnp.sum(jnp.concatenate(early + late + [blank], axis=0), axis=1, keepdims=True)
    row = lax.broadcasted_iota(jnp.int32, (8, 128), 0)
    lane = lax.broadcasted_iota(jnp.int32, (8, 128), 1)
    flat = jnp.sum(jnp.where(row == lane, sums, 0.0), axis=0, keepdims=True)
    gs[...] = flat
    ggat[me] = flat

    def g_copy(d):
        return send(gs, ggat.at[me], sga.at[d], rga.at[me], lax.rem(me + d, n))

    def g_arrived(d):
        q = lax.rem(me + d, n)
        return send(gs, ggat.at[q], sga.at[d], rga.at[q], q)

    for d in range(1, n):
        g_copy(d).start()
    for d in range(1, n):
        g_arrived(d).wait_recv()
    total = jnp.sum(ggat[...], axis=0)
    g01, g11, g02, g12, g22 = (total[:, j : j + 1] for j in range(1, 6))
    ratio = g12 / g11
    c2 = (g02 - ratio * g01) / (g22 - ratio * g12)
    c1 = g01 / g11 - ratio * c2
    coef[0:1, :] = jnp.broadcast_to(c1, (1, 128))
    coef[1:2, :] = jnp.broadcast_to(c2, (1, 128))

    for k in range(2):
        for d in range(1, block):
            a_copy(k, d).wait_send()
        for d in range(1, blocks):
            b_copy(k, d).wait_send()

        @pl.when(jnp.logical_and(p == block - 1, z > 0))
        def _():
            low_down(k).wait_send()

        @pl.when(jnp.logical_and(p == 0, z < blocks - 1))
        def _():
            low_up(k).wait_send()

        @pl.when(me > 0)
        def _():
            down(k).wait_send()

        @pl.when(me < n - 1)
        def _():
            up(k).wait_send()

    for d in range(1, n):
        g_copy(d).wait_send()


def finish(r, u1, u2, w1, w2, coef, x_hbm, res_hbm, xo, ro, out_sem):
    layers, rows, depth = r.shape
    step = 32
    c1 = coef[0:1, 0:1]
    c2 = coef[1:2, 0:1]
    outs = []
    for l in range(layers):
        for y in range(0, rows, step):
            a = PAD + y
            xo[l, y : y + step, :] = (
                c1 * u1[l + 1, a : a + step, :] + c2 * u2[l + 1, a : a + step, :]
            )
        c = pltpu.make_async_copy(xo.at[l], x_hbm.at[l], out_sem.at[0, l])
        c.start()
        outs.append(c)
    for l in range(layers):
        for y in range(0, rows, step):
            ro[l, y : y + step, :] = (
                r[l, y : y + step, :]
                - c1 * w1[l, y : y + step, :] - c2 * w2[l, y : y + step, :]
            )
        c = pltpu.make_async_copy(ro.at[l], res_hbm.at[l], out_sem.at[1, l])
        c.start()
        outs.append(c)
    for c in outs:
        c.wait()


def on_device(right_side, sigma, wind, local_inverse, basis_y, basis_z, gamma):
    n = lax.axis_size("sub")
    block = min(8, n)
    blocks = n // block
    layers, rows, depth = right_side.shape
    ky = basis_y.shape[1]
    kz = basis_z.shape[1]
    levels = gamma.shape[0]
    f32 = jnp.float32
    packed = (ky // 2, 2 * kz)
    cube = pltpu.VMEM((layers, rows, depth), f32)
    padded = pltpu.VMEM((layers + 2, rows + 2 * PAD, depth), f32)
    dma = pltpu.SemaphoreType.DMA
    scratch = [
        cube, cube,
        pltpu.VMEM((1, depth, depth), f32),
        pltpu.VMEM((ky, rows), f32),
        pltpu.VMEM((kz, depth), f32),
        pltpu.VMEM(gamma.shape, f32),
        pltpu.VMEM((depth, depth), jnp.bfloat16),
        pltpu.VMEM((depth, depth), jnp.bfloat16),
        pltpu.VMEM((2, 2, rows, depth), f32),
        pltpu.VMEM((2, 2, rows, depth), f32),
        pltpu.VMEM((2,) + packed, f32),
        pltpu.VMEM((2, block) + packed, f32),
        pltpu.VMEM((2,) + packed, f32),
        pltpu.VMEM((2, blocks) + packed, f32),
        pltpu.VMEM((2, 2) + packed, f32),
        pltpu.VMEM((2, 2) + packed, f32),
        pltpu.VMEM((3,) + packed, f32),
        pltpu.VMEM((1, 128), f32),
        pltpu.VMEM((n, 1, 128), f32),
        dma((7,)),
        dma((2, block)), dma((2, block)),
        dma((2, blocks)), dma((2, blocks)),
        dma((2, 2)), dma((2, 2)),
        dma((2, 2)), dma((2, 2)),
        dma((n,)), dma((n,)),
    ]
    hbm = pl.BlockSpec(memory_space=pltpu.HBM)
    vmem = pl.BlockSpec(memory_space=pltpu.VMEM)
    out = jax.ShapeDtypeStruct(right_side.shape, f32)
    pieces = pl.pallas_call(
        functools.partial(kernel, n, block),
        out_shape=(cube, padded, padded, cube, cube, pltpu.VMEM((8, 128), f32)),
        in_specs=[hbm] * 7,
        out_specs=(vmem,) * 6,
        scratch_shapes=scratch,
        compiler_params=pltpu.CompilerParams(
            collective_id=0, has_side_effects=True, vmem_limit_bytes=50 * 2**20,
        ),
        name="gmres",
    )(right_side, sigma, wind, local_inverse, basis_y.T, basis_z.T, gamma)
    return pl.pallas_call(
        finish,
        out_shape=(out, out),
        in_specs=[vmem] * 6,
        out_specs=(hbm, hbm),
        scratch_shapes=[cube, cube, dma((2, layers))],
        compiler_params=pltpu.CompilerParams(vmem_limit_bytes=24 * 2**20),
        name="finish",
    )(*pieces)


def solution(mesh):
    placed = (
        P("sub", None, None),
        P("sub", None, None),
        P("sub", None, None),
        P("sub", None, None),
        P(),
        P(),
        P(),
    )
    return jax.shard_map(
        on_device,
        mesh=mesh,
        in_specs=placed,
        out_specs=(P("sub", None, None), P("sub", None, None)),
        check_vma=False,
    )
```

```python
import functools

import jax
import jax.numpy as jnp
from jax import lax
from jax.experimental import pallas as pl
from jax.experimental.pallas import tpu as pltpu
from jax.sharding import PartitionSpec as P

HIGH = lax.Precision.HIGHEST
MESH = pl.DeviceIdType.MESH
PAD = 8


def split(x):
    hi = x.astype(jnp.bfloat16)
    lo = (x - hi.astype(jnp.float32)).astype(jnp.bfloat16)
    return hi, lo


def mm(a, b):
    return jnp.dot(a, b, preferred_element_type=jnp.float32)


def mt(a, b):
    return lax.dot_general(
        a, b, (((1,), (1,)), ((), ())), preferred_element_type=jnp.float32
    )


def tm(a, b):
    return lax.dot_general(
        a, b, (((0,), (0,)), ((), ())), preferred_element_type=jnp.float32
    )


def fold(x):
    part = jnp.sum(x, axis=0, keepdims=True)
    out = part[:, 0:128]
    for at in range(128, part.shape[1], 128):
        out = out + part[:, at : at + 128]
    return out


def kernel(
    n, block,
    r_hbm, sg_hbm, wd_hbm, li_hbm, by_hbm, bz_hbm, gm_hbm,
    r, u1, u2, w1, w2, coef,
    sg, wd, lf, by, bz, gm, lh, ll, by3, bz3, hs, hr,
    own, gat, tot, allb, low_s, low_r, nbr, gs, ggat,
    in_sem, sa, ra, sb, rb, se, re, sh, rh, sga, rga,
):
    layers, rows, depth = r.shape
    ky = by.shape[0]
    half = ky // 2
    kz = bz.shape[0]
    levels = gm.shape[0]
    blocks = n // block
    low_levels = block.bit_length() - 1
    me = lax.axis_index("sub")
    p = lax.rem(me, block)
    z = lax.div(me, block)
    us = (u1, u2)
    ws = (w1, w2)

    def load(i, src, dst):
        c = pltpu.make_async_copy(src, dst, in_sem.at[i])
        c.start()
        return c

    c_r = load(0, r_hbm, r)
    c_bz = load(1, bz_hbm, bz)
    c_by = load(2, by_hbm, by)
    c_l = load(3, li_hbm, lf)
    c_gm = load(4, gm_hbm, gm)
    c_sg = load(5, sg_hbm, sg)
    c_wd = load(6, wd_hbm, wd)

    barrier = pltpu.get_barrier_semaphore()
    in_block = [z * block + lax.rem(p + d, block) for d in range(1, block)]
    across = [lax.rem(z + d, blocks) * block + p for d in range(1, blocks)]
    first_cross = jnp.logical_and(p == 0, z > 0)
    last_cross = jnp.logical_and(p == block - 1, z < blocks - 1)

    def signal(target):
        pl.semaphore_signal(barrier, inc=1, device_id=(target,), device_id_type=MESH)

    for target in in_block + across:
        signal(target)

    @pl.when(first_cross)
    def _():
        signal(me - 1)

    @pl.when(last_cross)
    def _():
        signal(me + 1)

    zero_rows = jnp.zeros((PAD, depth), jnp.float32)
    for u in us:
        for l in range(1, layers + 1):
            u[l, 0:PAD, :] = zero_rows
            u[l, PAD + rows : PAD + rows + PAD, :] = zero_rows

    def send(src, dst, s, q, target):
        return pltpu.make_async_remote_copy(
            src_ref=src, dst_ref=dst, send_sem=s, recv_sem=q,
            device_id=(target,), device_id_type=MESH,
        )

    def project(k, field):
        summed = field[0]
        for l in range(1, layers):
            summed = summed + field[l]
        sh_, sl_ = split(summed)
        bh, bl = bz3[0:kz], bz3[2 * kz : 3 * kz]
        part = mt(sh_, bh) + mt(sl_, bh) + mt(sh_, bl)
        ph, pl_ = split(part)
        bh, bl = by3[0:ky], by3[2 * ky : 3 * ky]
        full = mm(bh, ph) + mm(bh, pl_) + mm(bl, ph)
        packed = jnp.concatenate([full[0:half], full[half:ky]], axis=1)
        own[k] = packed
        gat[k, p] = packed

    def a_copy(k, d):
        return send(own.at[k], gat.at[k, p], sa.at[k, d], ra.at[k, p], in_block[d - 1])

    def a_arrived(k, d):
        q = lax.rem(p + d, block)
        return send(own.at[k], gat.at[k, q], sa.at[k, d], ra.at[k, q], in_block[d - 1])

    def b_copy(k, d):
        return send(tot.at[k], allb.at[k, z], sb.at[k, d], rb.at[k, z], across[d - 1])

    def b_arrived(k, d):
        q = lax.rem(z + d, blocks)
        return send(tot.at[k], allb.at[k, q], sb.at[k, d], rb.at[k, q], across[d - 1])

    def down(k):
        return send(hs.at[k, 0], hr.at[k, 1], sh.at[k, 0], rh.at[k, 1], me - 1)

    def up(k):
        return send(hs.at[k, 1], hr.at[k, 0], sh.at[k, 1], rh.at[k, 0], me + 1)

    def low_down(k):
        return send(low_s.at[k, 0], low_r.at[k, 1], se.at[k, 0], re.at[k, 1], me - block)

    def low_up(k):
        return send(low_s.at[k, 1], low_r.at[k, 0], se.at[k, 1], re.at[k, 0], me + block)

    def local(x):
        xh, xl = split(x)
        return mm(xh, lh[...]) + mm(xl, lh[...]) + mm(xh, ll[...])

    def factor(level):
        g = gm[level]
        return jnp.concatenate([g[0:half], g[half:ky]], axis=1) * (
            (layers * 2 ** (level + 1)) ** -0.5
        )

    def low_part(k, q, upper):
        out = None
        for level in range(low_levels):
            width = 2 ** (level + 1)
            start = lax.div(q, width) * width
            if width == block:
                acc = tot[k]
            else:
                acc = gat[k, start]
                for j in range(1, width):
                    acc = acc + gat[k, start + j]
            term = upper[level] * acc
            out = term if out is None else out + term
        return out

    def high_part(k, zz, upper):
        out = jnp.zeros(tot.shape[1:], jnp.float32)
        for level in range(low_levels, levels):
            width = 2 ** (level + 1) // block
            start = lax.div(zz, width) * width
            acc = allb[k, start]
            for j in range(1, width):
                acc = acc + allb[k, start + j]
            out = out + upper[level] * acc
        return out

    def edges(k, field):
        first = local(field[0])
        hs[k, 0] = first
        us[k][1, PAD : PAD + rows, :] = first
        last = local(field[layers - 1])
        hs[k, 1] = last
        us[k][layers, PAD : PAD + rows, :] = last

    def send_edges(k):
        @pl.when(me > 0)
        def _():
            down(k).start()

        @pl.when(me < n - 1)
        def _():
            up(k).start()

    def middle(k, field):
        for l in range(1, layers - 1):
            us[k][l + 1, PAD : PAD + rows, :] = local(field[l])

    def exchange(k):
        fac = [factor(level) for level in range(levels)]
        for d in range(1, block):
            a_arrived(k, d).wait_recv()
        acc = gat[k, 0]
        for j in range(1, block):
            acc = acc + gat[k, j]
        tot[k] = acc
        allb[k, z] = acc
        for d in range(1, blocks):
            b_copy(k, d).start()

        @pl.when(jnp.logical_and(p == block - 1, z > 0))
        def _():
            low_s[k, 0] = low_part(k, 0, fac)
            low_down(k).start()

        @pl.when(jnp.logical_and(p == 0, z < blocks - 1))
        def _():
            low_s[k, 1] = low_part(k, block - 1, fac)
            low_up(k).start()

        nbr[1] = low_part(k, p, fac)

        @pl.when(p > 0)
        def _():
            nbr[0] = low_part(k, p - 1, fac)

        @pl.when(p < block - 1)
        def _():
            nbr[2] = low_part(k, p + 1, fac)

        @pl.when(jnp.logical_and(p == 0, z == 0))
        def _():
            nbr[0] = jnp.zeros(nbr.shape[1:], jnp.float32)

        @pl.when(jnp.logical_and(p == block - 1, z == blocks - 1))
        def _():
            nbr[2] = jnp.zeros(nbr.shape[1:], jnp.float32)

        for d in range(1, blocks):
            b_arrived(k, d).wait_recv()

        @pl.when(first_cross)
        def _():
            low_up(k).wait_recv()
            nbr[0] = low_r[k, 0]

        @pl.when(last_cross)
        def _():
            low_down(k).wait_recv()
            nbr[2] = low_r[k, 1]

        here = high_part(k, z, fac)
        before = high_part(k, lax.div(lax.rem(me + n - 1, n), block), fac)
        after = high_part(k, lax.div(lax.rem(me + 1, n), block), fac)
        three = []
        for c in (nbr[0] + before, nbr[1] + here, nbr[2] + after):
            three += [c[:, 0:kz], c[:, kz : 2 * kz]]
        stack = jnp.concatenate(three, axis=0)
        th, tl = split(stack)
        back = mm(jnp.concatenate([th, tl, th], axis=1), bz3[...])
        th, tl = split(back)
        spreads = []
        for j in range(3):
            piece = slice(j * ky, (j + 1) * ky)
            spreads.append(
                tm(by3[...], jnp.concatenate([th[piece], tl[piece], th[piece]], axis=0))
            )
        u = us[k]
        mine = spreads[1]
        for l in range(1, layers + 1):
            u[l, PAD : PAD + rows, :] = u[l, PAD : PAD + rows, :] + mine
        u[0, PAD : PAD + rows, :] = jnp.where(me > 0, spreads[0], 0.0)
        u[layers + 1, PAD : PAD + rows, :] = jnp.where(me < n - 1, spreads[2], 0.0)

    step = 32

    def operator(k, l):
        u = us[k]
        col = lax.broadcasted_iota(jnp.int32, (step, depth), 1)
        for y in range(0, rows, step):
            a = PAD + y
            c = u[l + 1, a : a + step, :]
            hi = u[l + 2, a : a + step, :]
            lo = u[l, a : a + step, :]
            fwd = jnp.where(col == depth - 1, 0.0, pltpu.roll(c, depth - 1, 1))
            bwd = jnp.where(col == 0, 0.0, pltpu.roll(c, 1, 1))
            beside = (
                hi + lo + u[l + 1, a + 1 : a + step + 1, :]
                + u[l + 1, a - 1 : a + step - 1, :] + fwd + bwd
            )
            ws[k][l, y : y + step, :] = (
                (6.0 + sg[l, y : y + step, :]) * c - beside
                + wd[l, y : y + step, :] * (hi - lo)
            )

    def stencil(k):
        for l in range(layers):
            operator(k, l)

    def meet(k):
        w = ws[k]

        @pl.when(me > 0)
        def _():
            up(k).wait_recv()
            w[0] = w[0] - (1.0 + wd[0]) * hr[k, 0]

        @pl.when(me < n - 1)
        def _():
            down(k).wait_recv()
            w[layers - 1] = w[layers - 1] + (wd[layers - 1] - 1.0) * hr[k, 1]

    def dots(pairs, which):
        out = []
        for a, b in pairs:
            acc = None
            for l in which:
                term = a[l] * b[l]
                acc = term if acc is None else acc + term
            out.append(fold(acc))
        return out

    def triple(src, dst):
        hi, lo = split(src[...])
        m = src.shape[0]
        dst[0:m] = hi
        dst[m : 2 * m] = hi
        dst[2 * m : 3 * m] = lo

    c_bz.wait()
    triple(bz, bz3)
    c_by.wait()
    triple(by, by3)
    c_r.wait()
    project(0, r)
    c_l.wait()
    big, small = split(lf[0])
    lh[...] = big
    ll[...] = small
    edges(0, r)
    extra = jnp.where(first_cross, 1, 0) + jnp.where(last_cross, 1, 0)
    pl.semaphore_wait(barrier, block - 1 + blocks - 1 + extra)
    for d in range(1, block):
        a_copy(0, d).start()
    middle(0, r)
    send_edges(0)
    c_gm.wait()
    exchange(0)
    c_sg.wait()
    c_wd.wait()
    stencil(0)
    meet(0)

    project(1, w1)
    for d in range(1, block):
        a_copy(1, d).start()
    edges(1, w1)
    middle(1, w1)
    send_edges(1)
    early = dots([(r, r), (r, w1), (w1, w1)], range(layers))
    exchange(1)
    stencil(1)
    pairs = [(r, w2), (w1, w2), (w2, w2)]
    inside = dots(pairs, range(1, layers - 1))
    meet(1)
    late = [i + o for i, o in zip(inside, dots(pairs, (0, layers - 1)))]
    blank = jnp.zeros((2, 128), jnp.float32)
    sums = jnp.sum(jnp.concatenate(early + late + [blank], axis=0), axis=1, keepdims=True)
    row = lax.broadcasted_iota(jnp.int32, (8, 128), 0)
    lane = lax.broadcasted_iota(jnp.int32, (8, 128), 1)
    flat = jnp.sum(jnp.where(row == lane, sums, 0.0), axis=0, keepdims=True)
    gs[...] = flat
    ggat[me] = flat

    def g_copy(d):
        return send(gs, ggat.at[me], sga.at[d], rga.at[me], lax.rem(me + d, n))

    def g_arrived(d):
        q = lax.rem(me + d, n)
        return send(gs, ggat.at[q], sga.at[d], rga.at[q], q)

    for d in range(1, n):
        g_copy(d).start()
    for d in range(1, n):
        g_arrived(d).wait_recv()
    total = jnp.sum(ggat[...], axis=0)
    g01, g11, g02, g12, g22 = (total[:, j : j + 1] for j in range(1, 6))
    ratio = g12 / g11
    c2 = (g02 - ratio * g01) / (g22 - ratio * g12)
    c1 = g01 / g11 - ratio * c2
    coef[0:1, :] = jnp.broadcast_to(c1, (1, 128))
    coef[1:2, :] = jnp.broadcast_to(c2, (1, 128))

    for k in range(2):
        for d in range(1, block):
            a_copy(k, d).wait_send()
        for d in range(1, blocks):
            b_copy(k, d).wait_send()

        @pl.when(jnp.logical_and(p == block - 1, z > 0))
        def _():
            low_down(k).wait_send()

        @pl.when(jnp.logical_and(p == 0, z < blocks - 1))
        def _():
            low_up(k).wait_send()

        @pl.when(me > 0)
        def _():
            down(k).wait_send()

        @pl.when(me < n - 1)
        def _():
            up(k).wait_send()

    for d in range(1, n):
        g_copy(d).wait_send()


def finish(r, u1, u2, w1, w2, coef, x_hbm, res_hbm, xo, ro, out_sem):
    layers, rows, depth = r.shape
    step = 32
    c1 = coef[0:1, 0:1]
    c2 = coef[1:2, 0:1]
    outs = []
    for l in range(layers):
        for y in range(0, rows, step):
            a = PAD + y
            xo[l, y : y + step, :] = (
                c1 * u1[l + 1, a : a + step, :] + c2 * u2[l + 1, a : a + step, :]
            )
        c = pltpu.make_async_copy(xo.at[l], x_hbm.at[l], out_sem.at[0, l])
        c.start()
        outs.append(c)
    for l in range(layers):
        for y in range(0, rows, step):
            ro[l, y : y + step, :] = (
                r[l, y : y + step, :]
                - c1 * w1[l, y : y + step, :] - c2 * w2[l, y : y + step, :]
            )
        c = pltpu.make_async_copy(ro.at[l], res_hbm.at[l], out_sem.at[1, l])
        c.start()
        outs.append(c)
    for c in outs:
        c.wait()


def on_device(right_side, sigma, wind, local_inverse, basis_y, basis_z, gamma):
    n = lax.axis_size("sub")
    block = min(8, n)
    blocks = n // block
    layers, rows, depth = right_side.shape
    ky = basis_y.shape[1]
    kz = basis_z.shape[1]
    levels = gamma.shape[0]
    f32 = jnp.float32
    packed = (ky // 2, 2 * kz)
    cube = pltpu.VMEM((layers, rows, depth), f32)
    padded = pltpu.VMEM((layers + 2, rows + 2 * PAD, depth), f32)
    dma = pltpu.SemaphoreType.DMA
    scratch = [
        cube, cube,
        pltpu.VMEM((1, depth, depth), f32),
        pltpu.VMEM((ky, rows), f32),
        pltpu.VMEM((kz, depth), f32),
        pltpu.VMEM(gamma.shape, f32),
        pltpu.VMEM((depth, depth), jnp.bfloat16),
        pltpu.VMEM((depth, depth), jnp.bfloat16),
        pltpu.VMEM((3 * ky, rows), jnp.bfloat16),
        pltpu.VMEM((3 * kz, depth), jnp.bfloat16),
        pltpu.VMEM((2, 2, rows, depth), f32),
        pltpu.VMEM((2, 2, rows, depth), f32),
        pltpu.VMEM((2,) + packed, f32),
        pltpu.VMEM((2, block) + packed, f32),
        pltpu.VMEM((2,) + packed, f32),
        pltpu.VMEM((2, blocks) + packed, f32),
        pltpu.VMEM((2, 2) + packed, f32),
        pltpu.VMEM((2, 2) + packed, f32),
        pltpu.VMEM((3,) + packed, f32),
        pltpu.VMEM((1, 128), f32),
        pltpu.VMEM((n, 1, 128), f32),
        dma((7,)),
        dma((2, block)), dma((2, block)),
        dma((2, blocks)), dma((2, blocks)),
        dma((2, 2)), dma((2, 2)),
        dma((2, 2)), dma((2, 2)),
        dma((n,)), dma((n,)),
    ]
    hbm = pl.BlockSpec(memory_space=pltpu.HBM)
    vmem = pl.BlockSpec(memory_space=pltpu.VMEM)
    out = jax.ShapeDtypeStruct(right_side.shape, f32)
    pieces = pl.pallas_call(
        functools.partial(kernel, n, block),
        out_shape=(cube, padded, padded, cube, cube, pltpu.VMEM((8, 128), f32)),
        in_specs=[hbm] * 7,
        out_specs=(vmem,) * 6,
        scratch_shapes=scratch,
        compiler_params=pltpu.CompilerParams(
            collective_id=0, has_side_effects=True, vmem_limit_bytes=50 * 2**20,
        ),
        name="gmres",
    )(right_side, sigma, wind, local_inverse, basis_y.T, basis_z.T, gamma)
    return pl.pallas_call(
        finish,
        out_shape=(out, out),
        in_specs=[vmem] * 6,
        out_specs=(hbm, hbm),
        scratch_shapes=[cube, cube, dma((2, layers))],
        compiler_params=pltpu.CompilerParams(vmem_limit_bytes=24 * 2**20),
        name="finish",
    )(*pieces)


def solution(mesh):
    placed = (
        P("sub", None, None),
        P("sub", None, None),
        P("sub", None, None),
        P("sub", None, None),
        P(),
        P(),
        P(),
    )
    return jax.shard_map(
        on_device,
        mesh=mesh,
        in_specs=placed,
        out_specs=(P("sub", None, None), P("sub", None, None)),
        check_vma=False,
    )
```

```python
import functools

import jax
import jax.numpy as jnp
from jax import lax
from jax.experimental import pallas as pl
from jax.experimental.pallas import tpu as pltpu
from jax.sharding import PartitionSpec as P

HIGH = lax.Precision.HIGHEST
MESH = pl.DeviceIdType.MESH
PAD = 8


def split(x):
    hi = x.astype(jnp.bfloat16)
    lo = (x - hi.astype(jnp.float32)).astype(jnp.bfloat16)
    return hi, lo


def mm(a, b):
    return jnp.dot(a, b, preferred_element_type=jnp.float32)


def mt(a, b):
    return lax.dot_general(
        a, b, (((1,), (1,)), ((), ())), preferred_element_type=jnp.float32
    )


def tm(a, b):
    return lax.dot_general(
        a, b, (((0,), (0,)), ((), ())), preferred_element_type=jnp.float32
    )


def fold(x):
    part = jnp.sum(x, axis=0, keepdims=True)
    out = part[:, 0:128]
    for at in range(128, part.shape[1], 128):
        out = out + part[:, at : at + 128]
    return out


def kernel(
    n, block,
    r_hbm, sg_hbm, wd_hbm, li_hbm, by_hbm, bz_hbm, gm_hbm,
    r, u1, u2, w1, w2, coef,
    sg, wd, lf, by, bz, gm, lh, ll, by3, bz3, hs, hr,
    own, gat, tot, allb, low_s, low_r, nbr, gs, ggat,
    in_sem, sa, ra, sb, rb, se, re, sh, rh, sga, rga,
):
    layers, rows, depth = r.shape
    ky = by.shape[0]
    half = ky // 2
    kz = bz.shape[0]
    levels = gm.shape[0]
    blocks = n // block
    low_levels = block.bit_length() - 1
    me = lax.axis_index("sub")
    p = lax.rem(me, block)
    z = lax.div(me, block)
    us = (u1, u2)
    ws = (w1, w2)

    def load(i, src, dst):
        c = pltpu.make_async_copy(src, dst, in_sem.at[i])
        c.start()
        return c

    c_r = load(0, r_hbm, r)
    c_bz = load(1, bz_hbm, bz)
    c_by = load(2, by_hbm, by)
    c_l = load(3, li_hbm, lf)
    c_gm = load(4, gm_hbm, gm)

    barrier = pltpu.get_barrier_semaphore()
    in_block = [z * block + lax.rem(p + d, block) for d in range(1, block)]
    across = [lax.rem(z + d, blocks) * block + p for d in range(1, blocks)]
    first_cross = jnp.logical_and(p == 0, z > 0)
    last_cross = jnp.logical_and(p == block - 1, z < blocks - 1)

    def signal(target):
        pl.semaphore_signal(barrier, inc=1, device_id=(target,), device_id_type=MESH)

    for target in in_block + across:
        signal(target)

    @pl.when(first_cross)
    def _():
        signal(me - 1)

    @pl.when(last_cross)
    def _():
        signal(me + 1)

    zero_rows = jnp.zeros((PAD, depth), jnp.float32)
    for u in us:
        for l in range(1, layers + 1):
            u[l, 0:PAD, :] = zero_rows
            u[l, PAD + rows : PAD + rows + PAD, :] = zero_rows

    def send(src, dst, s, q, target):
        return pltpu.make_async_remote_copy(
            src_ref=src, dst_ref=dst, send_sem=s, recv_sem=q,
            device_id=(target,), device_id_type=MESH,
        )

    def project(k, field):
        summed = field[0]
        for l in range(1, layers):
            summed = summed + field[l]
        sh_, sl_ = split(summed)
        bh, bl = bz3[0:kz], bz3[2 * kz : 3 * kz]
        part = mt(sh_, bh) + mt(sl_, bh) + mt(sh_, bl)
        ph, pl_ = split(part)
        bh, bl = by3[0:ky], by3[2 * ky : 3 * ky]
        full = mm(bh, ph) + mm(bh, pl_) + mm(bl, ph)
        packed = jnp.concatenate([full[0:half], full[half:ky]], axis=1)
        own[k] = packed
        gat[k, p] = packed

    def a_copy(k, d):
        return send(own.at[k], gat.at[k, p], sa.at[k, d], ra.at[k, p], in_block[d - 1])

    def a_arrived(k, d):
        q = lax.rem(p + d, block)
        return send(own.at[k], gat.at[k, q], sa.at[k, d], ra.at[k, q], in_block[d - 1])

    def b_copy(k, d):
        return send(tot.at[k], allb.at[k, z], sb.at[k, d], rb.at[k, z], across[d - 1])

    def b_arrived(k, d):
        q = lax.rem(z + d, blocks)
        return send(tot.at[k], allb.at[k, q], sb.at[k, d], rb.at[k, q], across[d - 1])

    def down(k):
        return send(hs.at[k, 0], hr.at[k, 1], sh.at[k, 0], rh.at[k, 1], me - 1)

    def up(k):
        return send(hs.at[k, 1], hr.at[k, 0], sh.at[k, 1], rh.at[k, 0], me + 1)

    def low_down(k):
        return send(low_s.at[k, 0], low_r.at[k, 1], se.at[k, 0], re.at[k, 1], me - block)

    def low_up(k):
        return send(low_s.at[k, 1], low_r.at[k, 0], se.at[k, 1], re.at[k, 0], me + block)

    def local(x):
        xh, xl = split(x)
        return mm(xh, lh[...]) + mm(xl, lh[...]) + mm(xh, ll[...])

    def factor(level):
        g = gm[level]
        return jnp.concatenate([g[0:half], g[half:ky]], axis=1) * (
            (layers * 2 ** (level + 1)) ** -0.5
        )

    def low_part(k, q, upper):
        out = None
        for level in range(low_levels):
            width = 2 ** (level + 1)
            start = lax.div(q, width) * width
            if width == block:
                acc = tot[k]
            else:
                acc = gat[k, start]
                for j in range(1, width):
                    acc = acc + gat[k, start + j]
            term = upper[level] * acc
            out = term if out is None else out + term
        return out

    def high_part(k, zz, upper):
        out = jnp.zeros(tot.shape[1:], jnp.float32)
        for level in range(low_levels, levels):
            width = 2 ** (level + 1) // block
            start = lax.div(zz, width) * width
            acc = allb[k, start]
            for j in range(1, width):
                acc = acc + allb[k, start + j]
            out = out + upper[level] * acc
        return out

    def edges(k, field):
        first = local(field[0])
        hs[k, 0] = first

        @pl.when(me > 0)
        def _():
            down(k).start()

        us[k][1, PAD : PAD + rows, :] = first
        last = local(field[layers - 1])
        hs[k, 1] = last

        @pl.when(me < n - 1)
        def _():
            up(k).start()

        us[k][layers, PAD : PAD + rows, :] = last

    def middle(k, field):
        for l in range(1, layers - 1):
            us[k][l + 1, PAD : PAD + rows, :] = local(field[l])

    def exchange(k):
        fac = [factor(level) for level in range(levels)]
        for d in range(1, block):
            a_arrived(k, d).wait_recv()
        acc = gat[k, 0]
        for j in range(1, block):
            acc = acc + gat[k, j]
        tot[k] = acc
        allb[k, z] = acc
        for d in range(1, blocks):
            b_copy(k, d).start()

        @pl.when(jnp.logical_and(p == block - 1, z > 0))
        def _():
            low_s[k, 0] = low_part(k, 0, fac)
            low_down(k).start()

        @pl.when(jnp.logical_and(p == 0, z < blocks - 1))
        def _():
            low_s[k, 1] = low_part(k, block - 1, fac)
            low_up(k).start()

        nbr[1] = low_part(k, p, fac)

        @pl.when(p > 0)
        def _():
            nbr[0] = low_part(k, p - 1, fac)

        @pl.when(p < block - 1)
        def _():
            nbr[2] = low_part(k, p + 1, fac)

        @pl.when(jnp.logical_and(p == 0, z == 0))
        def _():
            nbr[0] = jnp.zeros(nbr.shape[1:], jnp.float32)

        @pl.when(jnp.logical_and(p == block - 1, z == blocks - 1))
        def _():
            nbr[2] = jnp.zeros(nbr.shape[1:], jnp.float32)

        for d in range(1, blocks):
            b_arrived(k, d).wait_recv()

        @pl.when(first_cross)
        def _():
            low_up(k).wait_recv()
            nbr[0] = low_r[k, 0]

        @pl.when(last_cross)
        def _():
            low_down(k).wait_recv()
            nbr[2] = low_r[k, 1]

        here = high_part(k, z, fac)
        before = high_part(k, lax.div(lax.rem(me + n - 1, n), block), fac)
        after = high_part(k, lax.div(lax.rem(me + 1, n), block), fac)
        three = []
        for c in (nbr[0] + before, nbr[1] + here, nbr[2] + after):
            three += [c[:, 0:kz], c[:, kz : 2 * kz]]
        stack = jnp.concatenate(three, axis=0)
        th, tl = split(stack)
        back = mm(jnp.concatenate([th, tl, th], axis=1), bz3[...])
        th, tl = split(back)
        spreads = []
        for j in range(3):
            piece = slice(j * ky, (j + 1) * ky)
            spreads.append(
                tm(by3[...], jnp.concatenate([th[piece], tl[piece], th[piece]], axis=0))
            )
        u = us[k]
        mine = spreads[1]
        for l in range(1, layers + 1):
            u[l, PAD : PAD + rows, :] = u[l, PAD : PAD + rows, :] + mine
        u[0, PAD : PAD + rows, :] = jnp.where(me > 0, spreads[0], 0.0)
        u[layers + 1, PAD : PAD + rows, :] = jnp.where(me < n - 1, spreads[2], 0.0)

    step = 32

    def operator(k, l):
        u = us[k]
        col = lax.broadcasted_iota(jnp.int32, (step, depth), 1)
        for y in range(0, rows, step):
            a = PAD + y
            c = u[l + 1, a : a + step, :]
            hi = u[l + 2, a : a + step, :]
            lo = u[l, a : a + step, :]
            fwd = jnp.where(col == depth - 1, 0.0, pltpu.roll(c, depth - 1, 1))
            bwd = jnp.where(col == 0, 0.0, pltpu.roll(c, 1, 1))
            beside = (
                hi + lo + u[l + 1, a + 1 : a + step + 1, :]
                + u[l + 1, a - 1 : a + step - 1, :] + fwd + bwd
            )
            ws[k][l, y : y + step, :] = (
                (6.0 + sg[l, y : y + step, :]) * c - beside
                + wd[l, y : y + step, :] * (hi - lo)
            )

    def stencil(k):
        for l in range(layers):
            operator(k, l)

    def meet(k):
        w = ws[k]

        @pl.when(me > 0)
        def _():
            up(k).wait_recv()
            w[0] = w[0] - (1.0 + wd[0]) * hr[k, 0]

        @pl.when(me < n - 1)
        def _():
            down(k).wait_recv()
            w[layers - 1] = w[layers - 1] + (wd[layers - 1] - 1.0) * hr[k, 1]

    def dots(pairs, which):
        out = []
        for a, b in pairs:
            acc = None
            for l in which:
                term = a[l] * b[l]
                acc = term if acc is None else acc + term
            out.append(fold(acc))
        return out

    def triple(src, dst):
        hi, lo = split(src[...])
        m = src.shape[0]
        dst[0:m] = hi
        dst[m : 2 * m] = hi
        dst[2 * m : 3 * m] = lo

    c_bz.wait()
    triple(bz, bz3)
    c_by.wait()
    triple(by, by3)
    c_r.wait()
    project(0, r)
    extra = jnp.where(first_cross, 1, 0) + jnp.where(last_cross, 1, 0)
    pl.semaphore_wait(barrier, block - 1 + blocks - 1 + extra)
    for d in range(1, block):
        a_copy(0, d).start()
    c_l.wait()
    c_sg = load(5, sg_hbm, sg)
    c_wd = load(6, wd_hbm, wd)
    big, small = split(lf[0])
    lh[...] = big
    ll[...] = small
    edges(0, r)
    middle(0, r)
    c_gm.wait()
    exchange(0)
    c_sg.wait()
    c_wd.wait()
    stencil(0)
    meet(0)

    project(1, w1)
    for d in range(1, block):
        a_copy(1, d).start()
    edges(1, w1)
    middle(1, w1)
    early = dots([(r, r), (r, w1), (w1, w1)], range(layers))
    exchange(1)
    stencil(1)
    pairs = [(r, w2), (w1, w2), (w2, w2)]
    inside = dots(pairs, range(1, layers - 1))
    meet(1)
    late = [i + o for i, o in zip(inside, dots(pairs, (0, layers - 1)))]
    blank = jnp.zeros((2, 128), jnp.float32)
    sums = jnp.sum(jnp.concatenate(early + late + [blank], axis=0), axis=1, keepdims=True)
    row = lax.broadcasted_iota(jnp.int32, (8, 128), 0)
    lane = lax.broadcasted_iota(jnp.int32, (8, 128), 1)
    flat = jnp.sum(jnp.where(row == lane, sums, 0.0), axis=0, keepdims=True)
    gs[...] = flat
    ggat[me] = flat

    def g_copy(d):
        return send(gs, ggat.at[me], sga.at[d], rga.at[me], lax.rem(me + d, n))

    def g_arrived(d):
        q = lax.rem(me + d, n)
        return send(gs, ggat.at[q], sga.at[d], rga.at[q], q)

    for d in range(1, n):
        g_copy(d).start()
    for d in range(1, n):
        g_arrived(d).wait_recv()
    total = jnp.sum(ggat[...], axis=0)
    g01, g11, g02, g12, g22 = (total[:, j : j + 1] for j in range(1, 6))
    ratio = g12 / g11
    c2 = (g02 - ratio * g01) / (g22 - ratio * g12)
    c1 = g01 / g11 - ratio * c2
    coef[0:1, :] = jnp.broadcast_to(c1, (1, 128))
    coef[1:2, :] = jnp.broadcast_to(c2, (1, 128))

    for k in range(2):
        for d in range(1, block):
            a_copy(k, d).wait_send()
        for d in range(1, blocks):
            b_copy(k, d).wait_send()

        @pl.when(jnp.logical_and(p == block - 1, z > 0))
        def _():
            low_down(k).wait_send()

        @pl.when(jnp.logical_and(p == 0, z < blocks - 1))
        def _():
            low_up(k).wait_send()

        @pl.when(me > 0)
        def _():
            down(k).wait_send()

        @pl.when(me < n - 1)
        def _():
            up(k).wait_send()

    for d in range(1, n):
        g_copy(d).wait_send()


def finish(r, u1, u2, w1, w2, coef, x_hbm, res_hbm, xo, ro, out_sem):
    layers, rows, depth = r.shape
    step = 32
    c1 = coef[0:1, 0:1]
    c2 = coef[1:2, 0:1]
    outs = []
    for l in range(layers):
        for y in range(0, rows, step):
            a = PAD + y
            xo[l, y : y + step, :] = (
                c1 * u1[l + 1, a : a + step, :] + c2 * u2[l + 1, a : a + step, :]
            )
        c = pltpu.make_async_copy(xo.at[l], x_hbm.at[l], out_sem.at[0, l])
        c.start()
        outs.append(c)
    for l in range(layers):
        for y in range(0, rows, step):
            ro[l, y : y + step, :] = (
                r[l, y : y + step, :]
                - c1 * w1[l, y : y + step, :] - c2 * w2[l, y : y + step, :]
            )
        c = pltpu.make_async_copy(ro.at[l], res_hbm.at[l], out_sem.at[1, l])
        c.start()
        outs.append(c)
    for c in outs:
        c.wait()


def on_device(right_side, sigma, wind, local_inverse, basis_y, basis_z, gamma):
    n = lax.axis_size("sub")
    block = min(8, n)
    blocks = n // block
    layers, rows, depth = right_side.shape
    ky = basis_y.shape[1]
    kz = basis_z.shape[1]
    levels = gamma.shape[0]
    f32 = jnp.float32
    packed = (ky // 2, 2 * kz)
    cube = pltpu.VMEM((layers, rows, depth), f32)
    padded = pltpu.VMEM((layers + 2, rows + 2 * PAD, depth), f32)
    dma = pltpu.SemaphoreType.DMA
    scratch = [
        cube, cube,
        pltpu.VMEM((1, depth, depth), f32),
        pltpu.VMEM((ky, rows), f32),
        pltpu.VMEM((kz, depth), f32),
        pltpu.VMEM(gamma.shape, f32),
        pltpu.VMEM((depth, depth), jnp.bfloat16),
        pltpu.VMEM((depth, depth), jnp.bfloat16),
        pltpu.VMEM((3 * ky, rows), jnp.bfloat16),
        pltpu.VMEM((3 * kz, depth), jnp.bfloat16),
        pltpu.VMEM((2, 2, rows, depth), f32),
        pltpu.VMEM((2, 2, rows, depth), f32),
        pltpu.VMEM((2,) + packed, f32),
        pltpu.VMEM((2, block) + packed, f32),
        pltpu.VMEM((2,) + packed, f32),
        pltpu.VMEM((2, blocks) + packed, f32),
        pltpu.VMEM((2, 2) + packed, f32),
        pltpu.VMEM((2, 2) + packed, f32),
        pltpu.VMEM((3,) + packed, f32),
        pltpu.VMEM((1, 128), f32),
        pltpu.VMEM((n, 1, 128), f32),
        dma((7,)),
        dma((2, block)), dma((2, block)),
        dma((2, blocks)), dma((2, blocks)),
        dma((2, 2)), dma((2, 2)),
        dma((2, 2)), dma((2, 2)),
        dma((n,)), dma((n,)),
    ]
    hbm = pl.BlockSpec(memory_space=pltpu.HBM)
    vmem = pl.BlockSpec(memory_space=pltpu.VMEM)
    out = jax.ShapeDtypeStruct(right_side.shape, f32)
    pieces = pl.pallas_call(
        functools.partial(kernel, n, block),
        out_shape=(cube, padded, padded, cube, cube, pltpu.VMEM((8, 128), f32)),
        in_specs=[hbm] * 7,
        out_specs=(vmem,) * 6,
        scratch_shapes=scratch,
        compiler_params=pltpu.CompilerParams(
            collective_id=0, has_side_effects=True, vmem_limit_bytes=50 * 2**20,
        ),
        name="gmres",
    )(right_side, sigma, wind, local_inverse, basis_y.T, basis_z.T, gamma)
    return pl.pallas_call(
        finish,
        out_shape=(out, out),
        in_specs=[vmem] * 6,
        out_specs=(hbm, hbm),
        scratch_shapes=[cube, cube, dma((2, layers))],
        compiler_params=pltpu.CompilerParams(vmem_limit_bytes=24 * 2**20),
        name="finish",
    )(*pieces)


def solution(mesh):
    placed = (
        P("sub", None, None),
        P("sub", None, None),
        P("sub", None, None),
        P("sub", None, None),
        P(),
        P(),
        P(),
    )
    return jax.shard_map(
        on_device,
        mesh=mesh,
        in_specs=placed,
        out_specs=(P("sub", None, None), P("sub", None, None)),
        check_vma=False,
    )
```
